32 devices in a mesh: virt: 8 (over z, x), aux: 4 (over y, core).
Axes of the slice: x: 2, y: 2, z: 4, core: 2. Of those that a mesh axis runs over, the one named last changes fastest.
Arguments:
- three_index: bfloat16 [600, 5120], P('aux', 'virt'), may hold values from -0.0625 to 0.0625
- eps_occ: float32 [20], replicated, may hold values from -1.5 to -0.5
- eps_virt: float32 [256], replicated, may hold values from 0.3 to 3
Outputs:
- virt_energy: float32 [256], P('virt')
- pair_energy: float32 [20, 20], replicated
The draws below stay inside these ranges and needn't reach their ends.
All inputs are finite; a program needn't handle non-finite values.
Results may differ from the reference program's by a relative error of at most 0.0003.
Values may be sent and summed in bfloat16 or wider, within the bound.
A program may use at most 128 MiB of HBM per device.

```python
import jax
import jax.numpy as jnp
from jax import lax

O = 20
VIRT_DEV = 32
VIRT = 256
AUX = 600


def level_of(own_key, shape, split, low, largest):
    gain = 1.0
    for axis_at, blocks in split:
        steps = jax.random.uniform(jax.random.fold_in(jax.random.fold_in(own_key, 6), axis_at), (blocks,), jnp.float32, low / len(split), largest / len(split))
        gain = gain * jnp.repeat(jnp.exp(steps), shape[axis_at] // blocks).reshape((-1,) + (1,) * (len(shape) - 1 - axis_at))
    return gain


def scatter_about(key, dims, spread, limit, split=(), kind=jnp.bfloat16):
    result = jax.random.normal(key, dims, jnp.float32) * spread
    if len(split) > 0:
        result = level_of(key, dims, split, -0.22, 0.18) * result
    return jnp.clip(result, min=-limit, max=limit).astype(kind)


def setup_inputs(seed: int = 0) -> dict:
    splits = jax.random.split(jax.random.key(seed), 4)
    three_index = scatter_about(splits[0], (AUX, VIRT * O), 0.011, 0.0625, ((0, 4), (1, 8)))
    eps_occ = jnp.clip(jax.random.uniform(splits[1], (O,), jnp.float32, -1.5, -0.5), -1.5, -0.5)
    eps_virt = jnp.clip(jax.random.uniform(splits[2], (VIRT,), jnp.float32, 0.3, 3.0), 0.3, 3.0)
    return {"three_index": three_index, "eps_occ": eps_occ, "eps_virt": eps_virt}


def reference(three_index, eps_occ, eps_virt):
    block_count = VIRT // VIRT_DEV
    widened = three_index.astype(jnp.float32).reshape(AUX, VIRT, O)

    def one_block(which):
        offset = (which * VIRT_DEV).astype(jnp.int32)
        left_rows = lax.dynamic_slice_in_dim(widened, offset, VIRT_DEV, 1)
        integrals = jnp.einsum("pai,pbj->iajb", left_rows, widened, precision=lax.Precision.HIGHEST)
        eps_own = lax.dynamic_slice_in_dim(eps_virt, offset, VIRT_DEV)
        denominator = (eps_occ[:, None, None, None] + eps_occ[None, None, :, None]
                       - eps_own[None, :, None, None] - eps_virt[None, None, None, :])
        swapped = jnp.transpose(integrals, (2, 1, 0, 3))
        energy_terms = integrals * (2.0 * integrals - swapped) / denominator
        return jnp.sum(energy_terms, axis=(0, 2, 3)), jnp.sum(energy_terms, axis=(1, 3))

    virt_parts, pair_parts = lax.map(one_block, jnp.arange(block_count, dtype=jnp.int32))
    return virt_parts.reshape(VIRT), jnp.sum(pair_parts, axis=0)
```

```python
import functools

import jax
import jax.numpy as jnp
from jax import lax
from jax.experimental import pallas as pl
from jax.experimental.pallas import tpu as pltpu
from jax.sharding import PartitionSpec as P

MESH = pl.DeviceIdType.MESH
F32 = jnp.float32
BF16 = jnp.bfloat16
EXACT = lax.Precision.HIGHEST
LANES = 128
NT = (((1,), (1,)), ((), ()))
NN = (((1,), (0,)), ((), ()))


def distances(n_aux):
    return list(range(1, n_aux + 1, 2)) + list(range(2, n_aux + 1, 2))


def pick(table, at):
    got = jnp.int32(table[0])
    for k in range(1, len(table)):
        got = jnp.where(at == k, jnp.int32(table[k]), got)
    return got


def label_of(virt, n_virt):
    return lax.rem(virt, 2) * (n_virt // 2) + virt // 2


def virt_of(label, n_virt):
    half = n_virt // 2
    return lax.rem(label, half) * 2 + label // half


def kernel(
    n_virt, n_aux, occ,
    x_ref, occ_ref, virt_ref,
    share_ref, pair_ref,
    held, lhs, rhs, order, ints, sums, parts, message, slots,
    own_sem, send_sem, recv_sem, msg_send, msg_recv,
):
    rows, cols = x_ref.shape
    width = cols // occ
    groups = LANES // width
    supers = occ // groups
    n = n_virt * n_aux
    v = lax.axis_index("virt")
    p = lax.axis_index("aux")
    me = v * n_aux + p
    table = distances(n_aux)
    label = label_of(v, n_virt)
    other = virt_of(lax.rem(label + pick(table, p), n_virt), n_virt)
    diag = jnp.logical_and(p == n_aux - 1, label >= n_virt // 2)

    barrier = pltpu.get_barrier_semaphore()

    def greet(k, c):
        t = lax.rem(me + k, n)
        pl.semaphore_signal(
            barrier, inc=1,
            device_id={"virt": t // n_aux, "aux": lax.rem(t, n_aux)},
            device_id_type=MESH,
        )
        return c

    lax.fori_loop(1, n, greet, 0)
    own = pltpu.make_async_copy(x_ref, held.at[0, p], own_sem)
    own.start()
    pl.semaphore_wait(barrier, n - 1)

    copies = []
    for k in range(n_aux):
        q = lax.rem(p + k, n_aux)
        target = virt_of(lax.rem(label + n_virt - pick(table, q), n_virt), n_virt)
        copies.append(pltpu.make_async_remote_copy(
            src_ref=x_ref, dst_ref=held.at[1, p],
            send_sem=send_sem.at[1, k], recv_sem=recv_sem.at[1, p],
            device_id={"virt": target, "aux": q}, device_id_type=MESH,
        ))
    for k in range(1, n_aux):
        q = lax.rem(p + k, n_aux)
        copies.append(pltpu.make_async_remote_copy(
            src_ref=x_ref, dst_ref=held.at[0, p],
            send_sem=send_sem.at[0, k], recv_sem=recv_sem.at[0, p],
            device_id={"virt": v, "aux": q}, device_id_type=MESH,
        ))
    for copy in copies:
        copy.start()

    def arrived(side, q):
        pltpu.make_async_copy(
            held.at[side, q], held.at[side, q], recv_sem.at[side, q]
        ).wait()

    row = lax.broadcasted_iota(jnp.int32, (cols, cols), 0)
    col = lax.broadcasted_iota(jnp.int32, (cols, cols), 1)
    hit = col == lax.rem(row, width) * occ + row // width
    order[...] = jnp.where(hit, 1.0, 0.0).astype(BF16)
    lhs[...] = jnp.zeros_like(lhs)
    rhs[...] = jnp.zeros_like(rhs)

    def turn(side, q):
        lhs[q, :, 0:rows] = lax.dot_general(
            order[...], held[side, q], NT, preferred_element_type=F32
        ).astype(BF16)

    own.wait()
    turn(0, p)

    def take(k, c):
        q = lax.rem(p + k, n_aux)
        arrived(0, q)
        turn(0, q)
        return c

    lax.fori_loop(1, n_aux, take, 0)

    lane = lax.broadcasted_iota(jnp.int32, (1, LANES), 1)
    part = lane // width
    down = lax.broadcasted_iota(jnp.int32, (width, 1), 0)
    lane_in = lax.rem(lane, width)

    def eps_down(which):
        got = jnp.zeros((width, 1), F32)
        for k in range(width):
            got = jnp.where(down == k, virt_ref[which * width + k], got)
        return got

    def eps_across(which):
        got = jnp.zeros((1, LANES), F32)
        for k in range(width):
            got = jnp.where(lane_in == k, virt_ref[which * width + k], got)
        return got

    occ_lane = []
    for cj in range(supers):
        got = jnp.zeros((1, LANES), F32)
        for t in range(groups):
            got = jnp.where(part == t, occ_ref[cj * groups + t], got)
        occ_lane.append(got)

    tall = -(-occ // 8)
    sums[...] = jnp.zeros_like(sums)
    n_tiles = jnp.where(diag, 2, 1)
    r8 = lax.broadcasted_iota(jnp.int32, (8, LANES), 0)
    l8 = lax.broadcasted_iota(jnp.int32, (8, LANES), 1)
    free = tall * width

    def tile(t, c):
        last = t == n_tiles - 1
        source = jnp.where(diag, t, 1)

        def step(k, c2):
            q = lax.rem(p + k, n_aux)

            @pl.when(last)
            def _():
                arrived(1, q)

            @pl.when(t == 1)
            def _():
                turn(1, q)

            rhs[0:rows, :] = lax.dot_general(
                held[source, q], order[...], NT, preferred_element_type=F32
            ).astype(BF16)
            more = lax.dot_general(lhs[q], rhs[...], NN, preferred_element_type=F32)

            @pl.when(k == 0)
            def _():
                ints[...] = more

            @pl.when(k > 0)
            def _():
                ints[...] += more

            return c2

        lax.fori_loop(0, n_aux, step, 0)

        left = jnp.where(t == 0, v, other)
        right = jnp.where(source == 0, v, other)
        base = -(eps_down(left) + eps_across(right))
        total = jnp.zeros((width, LANES), F32)
        for ci in range(supers):
            for cj in range(ci, supers):
                turned = []
                for g in range(groups):
                    block = ints[pl.ds((cj * groups + g) * width, width), pl.ds(ci * LANES, LANES)]
                    turned.append([block if r == 0 else pltpu.roll(block, r * width, 1) for r in range(groups)])
                for s in range(groups):
                    i = ci * groups + s
                    direct = ints[pl.ds(i * width, width), pl.ds(cj * LANES, LANES)]
                    swapped = turned[0][(0 - s) % groups]
                    for g in range(1, groups):
                        swapped = jnp.where(part == g, turned[g][(g - s) % groups], swapped)
                    below = base + (occ_lane[cj] + occ_ref[i])
                    if ci == cj:
                        term = direct * (2.0 * direct - swapped) / below
                    else:
                        term = 2.0 * (direct * (direct - swapped) + swapped * swapped) / below
                    total = total + term
                    short = term[0:8]
                    for m in range(8, width, 8):
                        short = short + term[m:m + 8]
                    sums[i * 8:i * 8 + 8, cj * LANES:(cj + 1) * LANES] = short

        wide = lax.broadcasted_iota(jnp.int32, (cols, LANES), 0)
        thin = lax.broadcasted_iota(jnp.int32, (cols, LANES), 1)
        fold = jnp.where(wide // width == thin, 1.0, 0.0)
        by_j = lax.dot_general(sums[...], fold, NN, precision=EXACT, preferred_element_type=F32)
        ri = lax.broadcasted_iota(jnp.int32, (tall * 8, occ * 8), 0)
        rj = lax.broadcasted_iota(jnp.int32, (tall * 8, occ * 8), 1)
        by_ij = lax.dot_general(
            jnp.where(rj // 8 == ri, 1.0, 0.0), by_j, NN,
            precision=EXACT, preferred_element_type=F32,
        )
        packed = by_ij[0:8]
        for g in range(1, tall):
            packed = packed + pltpu.roll(by_ij[g * 8:g * 8 + 8], g * width, 1)
        pads = [jnp.zeros((free, LANES), F32), total]
        if free + width < LANES:
            pads.append(jnp.zeros((LANES - free - width, LANES), F32))
        spread = jnp.concatenate(pads, 0)
        by_row = lax.dot_general(
            jnp.ones((8, LANES), F32), spread, NT, precision=EXACT, preferred_element_type=F32)
        by_col = lax.dot_general(
            jnp.ones((8, width), F32), total, NN, precision=EXACT, preferred_element_type=F32)
        folded = by_col
        for g in range(1, groups):
            folded = folded + pltpu.roll(by_col, g * width, 1)
        half = jnp.where(diag, 0.5, 1.0)
        packed = packed * half
        both = (by_row + folded) * 0.5
        first = jnp.where(diag, jnp.where(t == 0, both, 0.0), by_row)
        second = jnp.where(diag, jnp.where(t == 1, both, 0.0), folded)
        out = jnp.where(l8 < free, packed, jnp.where(r8 == 0, first, jnp.where(r8 == 1, second, 0.0)))

        @pl.when(t == 0)
        def _():
            message[...] = out

        @pl.when(t == 1)
        def _():
            message[...] += out

        return c

    lax.fori_loop(0, n_tiles, tile, 0)

    def tell(k, c):
        t = lax.rem(me + k, n)
        pltpu.make_async_remote_copy(
            src_ref=message, dst_ref=slots.at[me],
            send_sem=msg_send, recv_sem=msg_recv,
            device_id={"virt": t // n_aux, "aux": lax.rem(t, n_aux)},
            device_id_type=MESH,
        ).start()
        return c

    lax.fori_loop(1, n, tell, 0)
    slots[me] = message[...]
    for copy in copies:
        copy.wait_send()
    everyone = slots.at[pl.ds(0, n - 1)]
    pltpu.make_async_copy(everyone, everyone, msg_send).wait()
    pltpu.make_async_copy(everyone, everyone, msg_recv).wait()

    keep = jnp.logical_or(l8 < free, r8 < 0)

    def add(k, acc):
        sv = k // n_aux
        so = virt_of(lax.rem(label_of(sv, n_virt) + pick(table, lax.rem(k, n_aux)), n_virt), n_virt)
        row0 = jnp.where(sv == v, 1.0, 0.0)
        row1 = jnp.where(so == v, 1.0, 0.0)
        weight = jnp.where(keep, 1.0, jnp.where(r8 == 0, row0, row1))
        return acc + slots[k] * weight

    done = lax.fori_loop(0, n, add, jnp.zeros((8, LANES), F32))
    share = done[0:1] + done[1:2]
    share_ref[...] = share[:, free:free + width]
    blocks = [done] + [pltpu.roll(done, LANES - g * width, 1) for g in range(1, tall)]
    square = jnp.concatenate(blocks + [jnp.zeros((LANES - 8 * tall, LANES), F32)], 0)
    square = jnp.where(lax.broadcasted_iota(jnp.int32, (LANES, LANES), 1) < occ, square, 0.0)
    pair = square + square.T
    pair_ref[...] = pair[0:occ, 0:occ]


def on_device(n_virt, n_aux, three_index, eps_occ, eps_virt):
    occ = eps_occ.shape[0]
    rows, cols = three_index.shape
    width = cols // occ
    padded = -(-rows // LANES) * LANES
    n = n_virt * n_aux
    vmem = pl.BlockSpec(memory_space=pltpu.VMEM)
    smem = pl.BlockSpec(memory_space=pltpu.SMEM)
    share, pair = pl.pallas_call(
        functools.partial(kernel, n_virt, n_aux, occ),
        out_shape=(
            jax.ShapeDtypeStruct((1, width), F32),
            jax.ShapeDtypeStruct((occ, occ), F32),
        ),
        in_specs=[vmem, smem, smem],
        out_specs=(vmem, vmem),
        scratch_shapes=[
            pltpu.VMEM((2, n_aux, rows, cols), BF16),
            pltpu.VMEM((n_aux, cols, padded), BF16),
            pltpu.VMEM((padded, cols), BF16),
            pltpu.VMEM((cols, cols), BF16),
            pltpu.VMEM((cols, cols), F32),
            pltpu.VMEM((occ * 8, cols), F32),
            pltpu.VMEM((8, LANES), F32),
            pltpu.VMEM((8, LANES), F32),
            pltpu.VMEM((n, 8, LANES), F32),
            pltpu.SemaphoreType.DMA,
            pltpu.SemaphoreType.DMA((2, n_aux)),
            pltpu.SemaphoreType.DMA((2, n_aux)),
            pltpu.SemaphoreType.DMA,
            pltpu.SemaphoreType.DMA,
        ],
        compiler_params=pltpu.CompilerParams(collective_id=0, has_side_effects=True),
    )(three_index, eps_occ, eps_virt)
    return share.reshape(width), pair


def solution(mesh):
    n_virt, n_aux = mesh.shape["virt"], mesh.shape["aux"]
    assert n_virt == 2 * n_aux
    in_specs = (P("aux", "virt"), P(), P())
    out_specs = (P("virt"), P())
    return jax.shard_map(
        functools.partial(on_device, n_virt, n_aux), mesh=mesh,
        in_specs=in_specs, out_specs=out_specs, check_vma=False,
    )
```

```python
import functools

import jax
import jax.numpy as jnp
from jax import lax
from jax.experimental import pallas as pl
from jax.experimental.pallas import tpu as pltpu
from jax.sharding import PartitionSpec as P

MESH = pl.DeviceIdType.MESH
F32 = jnp.float32
BF16 = jnp.bfloat16
EXACT = lax.Precision.HIGHEST
LANES = 128
NT = (((1,), (1,)), ((), ()))
NN = (((1,), (0,)), ((), ()))


def distances(n_aux):
    return list(range(1, n_aux + 1, 2)) + list(range(2, n_aux + 1, 2))


def pick(table, at):
    got = jnp.int32(table[0])
    for k in range(1, len(table)):
        got = jnp.where(at == k, jnp.int32(table[k]), got)
    return got


def label_of(virt, n_virt):
    return lax.rem(virt, 2) * (n_virt // 2) + virt // 2


def virt_of(label, n_virt):
    half = n_virt // 2
    return lax.rem(label, half) * 2 + label // half


def kernel(
    n_virt, n_aux, occ,
    x_ref, occ_ref, virt_ref,
    done_ref,
    held, lhs, rhs, order, order_t, ints, sums, parts, message, slots,
    own_sem, send_sem, recv_sem, msg_send, msg_recv,
):
    rows, cols = x_ref.shape
    pitch = -(-rows // 16) * 16
    width = cols // occ
    groups = LANES // width
    supers = occ // groups
    n = n_virt * n_aux
    v = lax.axis_index("virt")
    p = lax.axis_index("aux")
    me = v * n_aux + p
    table = distances(n_aux)
    label = label_of(v, n_virt)
    other = virt_of(lax.rem(label + pick(table, p), n_virt), n_virt)
    lower = label < n_virt // 2
    solo = jnp.logical_and(p == n_aux - 1, jnp.logical_not(lower))
    extra = jnp.logical_and(p == n_aux // 2 - 1, lower)

    barrier = pltpu.get_barrier_semaphore()

    def greet(k, c):
        t = lax.rem(me + k, n)
        pl.semaphore_signal(
            barrier, inc=1,
            device_id={"virt": t // n_aux, "aux": lax.rem(t, n_aux)},
            device_id_type=MESH,
        )
        return c

    lax.fori_loop(1, n, greet, 0)
    own = pltpu.make_async_copy(x_ref, held.at[0, p], own_sem)
    own.start()
    pl.semaphore_wait(barrier, n - 1)

    pairs = n_aux // 2

    def place(k):
        return lax.rem(p // 2 + k // 2, pairs) * 2 + lax.rem(p + k, 2)

    def share_own(k):
        return pltpu.make_async_remote_copy(
            src_ref=x_ref, dst_ref=held.at[0, p],
            send_sem=send_sem.at[0, k], recv_sem=recv_sem.at[0, p],
            device_id={"virt": v, "aux": place(k)}, device_id_type=MESH,
        )

    def hand_on(k):
        q = place(k)
        return pltpu.make_async_remote_copy(
            src_ref=held.at[0, q], dst_ref=held.at[0, q],
            send_sem=send_sem.at[2, k], recv_sem=recv_sem.at[0, q],
            device_id={"virt": v, "aux": place(1)}, device_id_type=MESH,
        )

    def share_other(k):
        q = place(k)
        target = lax.rem(label + n_virt - pick(table, q), n_virt)
        copy = pltpu.make_async_remote_copy(
            src_ref=x_ref, dst_ref=held.at[1, p],
            send_sem=send_sem.at[1, k], recv_sem=recv_sem.at[1, p],
            device_id={"virt": virt_of(target, n_virt), "aux": q}, device_id_type=MESH,
        )
        wanted = jnp.logical_or(q < n_aux - 1, target < n_virt // 2)
        return copy, wanted

    for k in list(range(2, n_aux, 2)) + [1]:
        share_own(k).start()
    for k in range(n_aux):
        copy, wanted = share_other(k)
        pl.when(wanted)(copy.start)

    def arrived(side, q):
        pltpu.make_async_copy(
            held.at[side, q], held.at[side, q], recv_sem.at[side, q]
        ).wait()

    row = lax.broadcasted_iota(jnp.int32, (cols, cols), 0)
    col = lax.broadcasted_iota(jnp.int32, (cols, cols), 1)
    hit = col == lax.rem(row, width) * occ + row // width
    order[...] = jnp.where(hit, 1.0, 0.0).astype(BF16)
    hit = row == lax.rem(col, width) * occ + col // width
    order_t[...] = jnp.where(hit, 1.0, 0.0).astype(BF16)
    lhs[...] = jnp.zeros_like(lhs)
    rhs[...] = jnp.zeros_like(rhs)

    def turn(k):
        lhs[:, k * pitch:k * pitch + rows] = lax.dot_general(
            order[...], held[0, place(k)], NT, preferred_element_type=F32
        ).astype(BF16)

    own.wait()
    turn(0)
    for k in range(2, n_aux, 2):
        arrived(0, place(k))
        hand_on(k).start()
        turn(k)
    for k in range(1, n_aux, 2):
        arrived(0, place(k))
        turn(k)

    lane = lax.broadcasted_iota(jnp.int32, (1, LANES), 1)
    part = lane // width
    down = lax.broadcasted_iota(jnp.int32, (width, 1), 0)
    lane_in = lax.rem(lane, width)

    def eps_down(which):
        got = jnp.zeros((width, 1), F32)
        for k in range(width):
            got = jnp.where(down == k, virt_ref[which * width + k], got)
        return got

    def eps_across(which):
        got = jnp.zeros((1, LANES), F32)
        for k in range(width):
            got = jnp.where(lane_in == k, virt_ref[which * width + k], got)
        return got

    occ_lane = []
    for cj in range(supers):
        got = jnp.zeros((1, LANES), F32)
        for t in range(groups):
            got = jnp.where(part == t, occ_ref[cj * groups + t], got)
        occ_lane.append(got)

    tall = -(-occ // 8)
    sums[...] = jnp.zeros_like(sums)
    n_tiles = jnp.where(extra, 2, 1)
    r8 = lax.broadcasted_iota(jnp.int32, (8, LANES), 0)
    l8 = lax.broadcasted_iota(jnp.int32, (8, LANES), 1)
    free = tall * width

    def tile(t, c):
        diag = jnp.logical_or(solo, jnp.logical_and(extra, t == 0))
        source = jnp.where(diag, 0, 1)

        for k in range(n_aux):

            @pl.when(source == 1)
            def _():
                arrived(1, place(k))

            rhs[k * pitch:k * pitch + rows, :] = lax.dot_general(
                held[source, place(k)], order_t[...], NN, preferred_element_type=F32
            ).astype(BF16)
        ints[...] = lax.dot_general(lhs[...], rhs[...], NN, preferred_element_type=F32)

        base = -(eps_down(v) + eps_across(jnp.where(diag, v, other)))
        total = jnp.zeros((width, LANES), F32)
        for ci in range(supers):
            for cj in range(ci, supers):
                turned = []
                for g in range(groups):
                    block = ints[pl.ds((cj * groups + g) * width, width), pl.ds(ci * LANES, LANES)]
                    turned.append([block if r == 0 else pltpu.roll(block, r * width, 1) for r in range(groups)])
                for s in range(groups):
                    i = ci * groups + s
                    direct = ints[pl.ds(i * width, width), pl.ds(cj * LANES, LANES)]
                    swapped = turned[0][(0 - s) % groups]
                    for g in range(1, groups):
                        swapped = jnp.where(part == g, turned[g][(g - s) % groups], swapped)
                    below = base + (occ_lane[cj] + occ_ref[i])
                    if ci == cj:
                        term = direct * (2.0 * direct - swapped) / below
                    else:
                        term = 2.0 * (direct * (direct - swapped) + swapped * swapped) / below
                    total = total + term
                    short = term[0:8]
                    for m in range(8, width, 8):
                        short = short + term[m:m + 8]
                    sums[i * 8:i * 8 + 8, cj * LANES:(cj + 1) * LANES] = short

        wide = lax.broadcasted_iota(jnp.int32, (cols, LANES), 0)
        thin = lax.broadcasted_iota(jnp.int32, (cols, LANES), 1)
        fold = jnp.where(wide // width == thin, 1.0, 0.0)
        by_j = lax.dot_general(sums[...], fold, NN, precision=EXACT, preferred_element_type=F32)
        ri = lax.broadcasted_iota(jnp.int32, (tall * 8, occ * 8), 0)
        rj = lax.broadcasted_iota(jnp.int32, (tall * 8, occ * 8), 1)
        by_ij = lax.dot_general(
            jnp.where(rj // 8 == ri, 1.0, 0.0), by_j, NN,
            precision=EXACT, preferred_element_type=F32,
        )
        packed = by_ij[0:8]
        for g in range(1, tall):
            packed = packed + pltpu.roll(by_ij[g * 8:g * 8 + 8], g * width, 1)
        pads = [jnp.zeros((free, LANES), F32), total]
        if free + width < LANES:
            pads.append(jnp.zeros((LANES - free - width, LANES), F32))
        spread = jnp.concatenate(pads, 0)
        by_row = lax.dot_general(
            jnp.ones((8, LANES), F32), spread, NT, precision=EXACT, preferred_element_type=F32)
        by_col = lax.dot_general(
            jnp.ones((8, width), F32), total, NN, precision=EXACT, preferred_element_type=F32)
        folded = by_col
        for g in range(1, groups):
            folded = folded + pltpu.roll(by_col, g * width, 1)
        packed = packed * jnp.where(diag, 0.5, 1.0)
        first = jnp.where(diag, (by_row + folded) * 0.5, by_row)
        second = jnp.where(diag, 0.0, folded)
        out = jnp.where(l8 < free, packed, jnp.where(r8 == 0, first, jnp.where(r8 == 1, second, 0.0)))

        @pl.when(t == 0)
        def _():
            message[...] = out

        @pl.when(t == 1)
        def _():
            message[...] += out

        return c

    lax.fori_loop(0, n_tiles, tile, 0)

    def tell(k, c):
        t = lax.rem(me + k, n)
        pltpu.make_async_remote_copy(
            src_ref=message, dst_ref=slots.at[me],
            send_sem=msg_send, recv_sem=msg_recv,
            device_id={"virt": t // n_aux, "aux": lax.rem(t, n_aux)},
            device_id_type=MESH,
        ).start()
        return c

    lax.fori_loop(1, n, tell, 0)
    slots[me] = message[...]
    for k in list(range(2, n_aux, 2)) + [1]:
        share_own(k).wait_send()
    for k in range(2, n_aux, 2):
        hand_on(k).wait_send()
    for k in range(n_aux):
        copy, wanted = share_other(k)
        pl.when(wanted)(copy.wait_send)
    everyone = slots.at[pl.ds(0, n - 1)]
    pltpu.make_async_copy(everyone, everyone, msg_send).wait()
    pltpu.make_async_copy(everyone, everyone, msg_recv).wait()

    keep = jnp.logical_or(l8 < free, r8 < 0)

    def add(k, acc):
        sv = k // n_aux
        so = virt_of(lax.rem(label_of(sv, n_virt) + pick(table, lax.rem(k, n_aux)), n_virt), n_virt)
        row0 = jnp.where(sv == v, 1.0, 0.0)
        row1 = jnp.where(so == v, 1.0, 0.0)
        weight = jnp.where(keep, 1.0, jnp.where(r8 == 0, row0, row1))
        return acc + slots[k] * weight

    done = lax.fori_loop(0, n, add, jnp.zeros((8, LANES), F32))
    done_ref[...] = done


def unpack(occ, width, done_ref, share_ref, pair_ref):
    tall = -(-occ // 8)
    free = tall * width
    done = done_ref[...]
    share = done[0:1] + done[1:2]
    share_ref[...] = share[0, free:free + width]
    blocks = [done] + [pltpu.roll(done, LANES - g * width, 1) for g in range(1, tall)]
    square = jnp.concatenate(blocks + [jnp.zeros((LANES - 8 * tall, LANES), F32)], 0)
    square = jnp.where(lax.broadcasted_iota(jnp.int32, (LANES, LANES), 1) < occ, square, 0.0)
    pair = square + square.T
    pair_ref[...] = pair[0:occ, 0:occ]


def on_device(n_virt, n_aux, three_index, eps_occ, eps_virt):
    occ = eps_occ.shape[0]
    rows, cols = three_index.shape
    width = cols // occ
    pitch = -(-rows // 16) * 16
    n = n_virt * n_aux
    vmem = pl.BlockSpec(memory_space=pltpu.VMEM)
    smem = pl.BlockSpec(memory_space=pltpu.SMEM)
    done = pl.pallas_call(
        functools.partial(kernel, n_virt, n_aux, occ),
        out_shape=jax.ShapeDtypeStruct((8, LANES), F32),
        in_specs=[vmem, smem, smem],
        out_specs=vmem,
        scratch_shapes=[
            pltpu.VMEM((2, n_aux, rows, cols), BF16),
            pltpu.VMEM((cols, n_aux * pitch), BF16),
            pltpu.VMEM((n_aux * pitch, cols), BF16),
            pltpu.VMEM((cols, cols), BF16),
            pltpu.VMEM((cols, cols), BF16),
            pltpu.VMEM((cols, cols), F32),
            pltpu.VMEM((occ * 8, cols), F32),
            pltpu.VMEM((8, LANES), F32),
            pltpu.VMEM((8, LANES), F32),
            pltpu.VMEM((n, 8, LANES), F32),
            pltpu.SemaphoreType.DMA,
            pltpu.SemaphoreType.DMA((3, n_aux)),
            pltpu.SemaphoreType.DMA((2, n_aux)),
            pltpu.SemaphoreType.DMA,
            pltpu.SemaphoreType.DMA,
        ],
        compiler_params=pltpu.CompilerParams(collective_id=0, has_side_effects=True),
    )(three_index, eps_occ, eps_virt)
    return pl.pallas_call(
        functools.partial(unpack, occ, width),
        out_shape=(
            jax.ShapeDtypeStruct((width,), F32),
            jax.ShapeDtypeStruct((occ, occ), F32),
        ),
        in_specs=[vmem],
        out_specs=(vmem, vmem),
    )(done)


def solution(mesh):
    n_virt, n_aux = mesh.shape["virt"], mesh.shape["aux"]
    assert n_virt == 2 * n_aux and n_aux % 2 == 0
    in_specs = (P("aux", "virt"), P(), P())
    out_specs = (P("virt"), P())
    return jax.shard_map(
        functools.partial(on_device, n_virt, n_aux), mesh=mesh,
        in_specs=in_specs, out_specs=out_specs, check_vma=False,
    )
```
